128 devices in a mesh: group: 16 (over y, x), tp: 8 (over z, core).
Axes of the slice: x: 4, y: 4, z: 4, core: 2. Of those that a mesh axis runs over, the one named last changes fastest.
Arguments:
- queries: bfloat16 [256, 8192], P('group', 'tp'), may hold values from -100 to 100
- cache_keys: bfloat16 [256, 512, 1024], P('group', None, 'tp'), may hold values from -6 to 6
- cache_values: bfloat16 [256, 512, 1024], P('group', None, 'tp'), may hold values from -6 to 6
- pool_keys: bfloat16 [32, 4096, 1024], P('group', None, 'tp'), may hold values from -6 to 6
- pool_values: bfloat16 [32, 4096, 1024], P('group', None, 'tp'), may hold values from -6 to 6
- row_lengths: int32 [256], P('group'), may hold values from 2 to 49664, as said below
- slot_owner: int32 [32], P('group'), may hold values from -1 to 255, as said below
- slot_fill: int32 [32], P('group'), may hold values from 0 to 4096, as said below
- free_counts: int32 [16], P('group'), may hold values from 0 to 2047
- out_weight: bfloat16 [8192, 8192], P('tp'), may hold values from -0.0625 to 0.0625
Outputs:
- mixed_out: bfloat16 [256, 8192], P('group', 'tp')
- total_free: int32 [1], replicated
The draws below stay inside these ranges and needn't reach their ends.
Inputs may be any that keep to these rules, and one draw needn't show every extreme that they name: `row_lengths`: A row of length over 512 has the rest of its positions in the slots it owns, so its length is 512 plus the sum of their slot_fill; other rows own no slot. `slot_owner`: each slot is free or holds one block of one row; slots may sit in any group, the row's own too. `slot_fill`: A free slot has fill 0, an owned one at least 2.
All inputs are finite; a program needn't handle non-finite values.
Results may differ from the reference program's by a relative error of at most 0.0066.
Values may be sent and summed in bfloat16 or wider, within the bound.
A program may use at most 128 MiB of HBM per device.

```python
import math
import jax
import jax.numpy as jnp
from jax import lax

D = 8192
HEADS = 64
KV_HEADS = 8
HEAD_DIM = 128
CAP = 512
BLOCK = 4096
LONG_BLOCKS = 12
GROUPS = 16
LONG_ROWS = 2
TOTAL_ROWS = 256
SLOTS_ALL = 32


def drawn_keys(key, drawn):
    return drawn


def draw_queries(key, part):
    drawn = jnp.clip(2.0 * jax.random.normal(jax.random.fold_in(key, 33), (TOTAL_ROWS, HEADS, HEAD_DIM), jnp.float32), -12.0, 12.0)
    return drawn.reshape(TOTAL_ROWS, HEADS * HEAD_DIM).astype(jnp.bfloat16)


def draw_cache_keys(key, part):
    drawn = jnp.clip(jax.random.normal(jax.random.fold_in(key, 31), (TOTAL_ROWS, CAP, KV_HEADS * HEAD_DIM), jnp.float32), -6.0, 6.0)
    return drawn_keys(key, drawn).astype(jnp.bfloat16)


def draw_pool_keys(key, part):
    drawn = jnp.clip(jax.random.normal(jax.random.fold_in(key, 32), (SLOTS_ALL, BLOCK, KV_HEADS * HEAD_DIM), jnp.float32), -6.0, 6.0)
    return drawn_keys(key, drawn).astype(jnp.bfloat16)


def layout(key):
    others = jax.random.permutation(jax.random.fold_in(key, 11), TOTAL_ROWS - 1)[:LONG_ROWS - 1].astype(jnp.int32)
    long_rows = jnp.concatenate([jnp.full((1,), TOTAL_ROWS - 1, jnp.int32), others])
    placed = jax.random.permutation(jax.random.fold_in(key, 12), SLOTS_ALL)[:LONG_ROWS * LONG_BLOCKS].astype(jnp.int32)
    last_fill = jax.random.randint(jax.random.fold_in(key, 13), (LONG_ROWS,), 2, BLOCK + 1).astype(jnp.int32)
    short_len = jax.random.randint(jax.random.fold_in(key, 14), (TOTAL_ROWS,), 2, CAP + 1).astype(jnp.int32)
    lengths = short_len.at[long_rows].set(CAP + (LONG_BLOCKS - 1) * BLOCK + last_fill)
    owners = jnp.full((SLOTS_ALL,), -1, jnp.int32).at[placed].set(jnp.repeat(long_rows, LONG_BLOCKS))
    block_fill = jnp.full((LONG_ROWS, LONG_BLOCKS), BLOCK, jnp.int32).at[:, LONG_BLOCKS - 1].set(last_fill).reshape(-1)
    filled = jnp.zeros((SLOTS_ALL,), jnp.int32).at[placed].set(block_fill)
    return (lengths, owners, filled)


def draw_row_lengths(key, part):
    return layout(key)[0]


def draw_slot_owner(key, part):
    return layout(key)[1]


def draw_slot_fill(key, part):
    return layout(key)[2]


def draw_free_counts(key, part):
    levels = jax.random.randint(jax.random.fold_in(key, 22), (GROUPS,), 1, 12).astype(jnp.int32)
    reach = jnp.left_shift(jnp.ones((GROUPS,), jnp.int32), levels)
    spread = jax.random.randint(jax.random.fold_in(key, 21), (GROUPS,), 0, 2048).astype(jnp.int32)
    spread = jnp.remainder(spread, reach).astype(jnp.int32)
    return spread.at[GROUPS - 1].set(2047).at[0].set(0).astype(jnp.int32)


def block_levels(rng, dims, shards, least, top_value):
    factor_of = 1.0
    for axis_at, shards_of in shards:
        steps = jax.random.uniform(jax.random.fold_in(jax.random.fold_in(rng, 6), axis_at), (shards_of,), jnp.float32, least / len(shards), top_value / len(shards))
        factor_of = factor_of * jnp.repeat(jnp.exp(steps), dims[axis_at] // shards_of).reshape((-1,) + (1,) * (len(dims) - 1 - axis_at))
    return factor_of


def noise(own_key, extent, scale, bound, cuts=(), kind=jnp.bfloat16):
    array = jax.random.normal(own_key, extent, jnp.float32) * scale
    if len(cuts) > 0:
        array = block_levels(own_key, extent, cuts, -0.22, 0.18) * array
    return jnp.clip(array, min=-bound, max=bound).astype(kind)


def setup_inputs(seed: int = 0) -> dict:
    splits = jax.random.split(jax.random.key(seed), 11)
    queries = draw_queries(jax.random.fold_in(splits[10], 71), 0)
    cache_keys = draw_cache_keys(jax.random.fold_in(splits[10], 71), 0)
    cache_values = noise(splits[2], (TOTAL_ROWS, CAP, KV_HEADS * HEAD_DIM), 1.0, 6.0, ((0, 16), (2, 8)))
    pool_keys = draw_pool_keys(jax.random.fold_in(splits[10], 71), 0)
    pool_values = noise(splits[4], (SLOTS_ALL, BLOCK, KV_HEADS * HEAD_DIM), 1.0, 6.0, ((0, 16), (2, 8)))
    row_lengths = draw_row_lengths(jax.random.fold_in(splits[10], 71), 0)
    slot_owner = draw_slot_owner(jax.random.fold_in(splits[10], 71), 0)
    slot_fill = draw_slot_fill(jax.random.fold_in(splits[10], 71), 0)
    free_counts = draw_free_counts(jax.random.fold_in(splits[10], 71), 0)
    out_weight = noise(splits[9], (HEADS * HEAD_DIM, D), (HEADS * HEAD_DIM) ** -0.5, 0.0625, ((0, 8),))
    return dict(queries=queries, cache_keys=cache_keys, cache_values=cache_values, pool_keys=pool_keys, pool_values=pool_values, row_lengths=row_lengths, slot_owner=slot_owner, slot_fill=slot_fill, free_counts=free_counts, out_weight=out_weight)


far_below = -1e+30

def partial_attention(queries, key_block, values, live_count):
    batch_rows, positions = (key_block.shape[0], key_block.shape[1])
    kv_heads = key_block.shape[2] // HEAD_DIM
    query_heads = queries.shape[1] // HEAD_DIM
    query_split = queries.reshape(batch_rows, kv_heads, query_heads // kv_heads, HEAD_DIM).astype(jnp.float32)
    key_split = key_block.reshape(batch_rows, positions, kv_heads, HEAD_DIM).astype(jnp.float32)
    value_split = values.reshape(batch_rows, positions, kv_heads, HEAD_DIM).astype(jnp.float32)
    scores = jnp.einsum('nkgd,nlkd->nkgl', query_split, key_split) / math.sqrt(HEAD_DIM)
    visible = (jnp.arange(positions, dtype=jnp.int32)[None, :] < live_count[:, None])[:, None, None, :]
    scores = jnp.where(visible, scores, far_below)
    highest = lax.optimization_barrier(jnp.max(scores, axis=-1))
    weights = jnp.where(visible, jnp.exp(scores - highest[..., None]), 0.0)
    weight_sum = lax.optimization_barrier(jnp.sum(weights, axis=-1))
    rounded = weights.astype(jnp.bfloat16).astype(jnp.float32)
    mixed = jnp.einsum('nkgl,nlkd->nkgd', rounded, value_split)
    return (highest.reshape(batch_rows, query_heads), weight_sum.reshape(batch_rows, query_heads), mixed.reshape(batch_rows, query_heads, HEAD_DIM))

def one_row(single):
    query_row, key_rows, value_rows, live_count = single
    highest, weight_sum, mixed = partial_attention(query_row[None], key_rows[None], value_rows[None], live_count[None])
    return (highest[0], weight_sum[0], mixed[0])

def reference(queries, cache_keys, cache_values, pool_keys, pool_values, row_lengths, slot_owner, slot_fill, free_counts, out_weight):
    local_high, local_total, local_mixed = lax.map(one_row, (queries, cache_keys, cache_values, jnp.minimum(row_lengths, CAP).astype(jnp.int32)))
    chosen = queries[jnp.maximum(slot_owner, 0).astype(jnp.int32)]
    slot_high, slot_total, slot_mixed = lax.map(one_row, (chosen, pool_keys, pool_values, slot_fill))
    row_count = queries.shape[0]
    matched = (jnp.arange(row_count, dtype=jnp.int32)[:, None] == slot_owner[None, :])[:, :, None]
    far_high = lax.optimization_barrier(jnp.max(jnp.where(matched, slot_high[None], far_below), axis=1))
    factor = jnp.where(matched, jnp.exp(slot_high[None] - far_high[:, None]), 0.0)
    far_total = lax.optimization_barrier(jnp.sum(factor * slot_total[None], axis=1))
    far_mixed = jnp.einsum('rsh,shd->rhd', factor, slot_mixed, precision=lax.Precision.HIGHEST)
    peak = jnp.maximum(local_high, far_high)
    near_scale = jnp.exp(local_high - peak)
    far_scale = jnp.exp(far_high - peak)
    attended = (near_scale[..., None] * local_mixed + far_scale[..., None] * far_mixed) / (near_scale * local_total + far_scale * far_total)[..., None]
    attended = attended.reshape(row_count, -1).astype(jnp.bfloat16)
    mixed_out = jnp.dot(attended, out_weight, preferred_element_type=jnp.float32).astype(jnp.bfloat16)
    total_free = jnp.sum(free_counts).astype(jnp.int32).reshape(1)
    return (mixed_out, total_free)
```

```python
import math

import jax
import jax.numpy as jnp
from jax import lax
from jax.experimental import pallas as pl
from jax.experimental.pallas import tpu as pltpu
from jax.sharding import PartitionSpec as P

MESH = pl.DeviceIdType.MESH
HEAD_DIM = 128
FAR_BELOW = -1e30
SCALE = math.log2(math.e) / math.sqrt(HEAD_DIM)

ROWS = 16
HEADS = 8
CAP = 512
SLOTS = 2
BLOCK = 4096
GROUPS = 16
TP = 8
WIDTH = HEADS * HEAD_DIM
COLUMNS = 1024
PAIRS = ROWS * HEADS
SLOT_PAIRS = SLOTS * HEADS

OFFSETS = sorted(
    ((dy, dx) for dy in range(4) for dx in range(4) if (dy, dx) != (0, 0)),
    key=lambda o: -(min(o[0], 4 - o[0]) + min(o[1], 4 - o[1])),
)


def dot_nt(a, b):
    return lax.dot_general(a, b, (((1,), (1,)), ((), ())), preferred_element_type=jnp.float32)


def dot(a, b, precision=None):
    return jnp.dot(a, b, preferred_element_type=jnp.float32, precision=precision)


def iota(shape, dim):
    return lax.broadcasted_iota(jnp.int32, shape, dim)


def kernel(
    q_hbm, ck_hbm, cv_hbm, pk_hbm, pv_hbm, len_hbm, own_hbm, fill_hbm, free_hbm, w_hbm,
    out_ref, free_ref,
    qall, ck, cv, pk, pv, w, qf, local_mixed, local_high, local_total, mixed_all, table_all,
    sent, arrived, lens, owns, fills, frees,
    load_sem, small_sem, w_sem, q_send, q_recv, m_send, m_recv, t_send, t_recv, o_send, o_recv,
):
    group = lax.axis_index("group")
    tp = lax.axis_index("tp")
    gy, gx = group // 4, group % 4
    peers = [((gy + dy) % 4) * 4 + (gx + dx) % 4 for dy, dx in OFFSETS]

    smalls = [
        pltpu.make_async_copy(src, dst, small_sem.at[i])
        for i, (src, dst) in enumerate(
            ((len_hbm, lens), (own_hbm, owns), (fill_hbm, fills), (free_hbm, frees))
        )
    ]
    loads = [
        pltpu.make_async_copy(src, dst, load_sem.at[i])
        for i, (src, dst) in enumerate(
            ((q_hbm, qall.at[group]), (ck_hbm, ck), (cv_hbm, cv), (pk_hbm, pk), (pv_hbm, pv))
        )
    ]

    def w_load(block):
        columns = pl.ds(pl.multiple_of(block * COLUMNS, COLUMNS), COLUMNS)
        return pltpu.make_async_copy(w_hbm.at[:, columns], w.at[block], w_sem.at[block])

    loads[0].start()
    barrier = pltpu.get_barrier_semaphore()
    for peer in peers:
        pl.semaphore_signal(barrier, inc=1, device_id={"group": peer}, device_id_type=MESH)
    for k in range(1, TP):
        pl.semaphore_signal(barrier, inc=1, device_id={"tp": (tp + k) % TP}, device_id_type=MESH)
    for copy in smalls:
        copy.start()
    for copy in loads[1:]:
        copy.start()
    for k in range(1, TP + 1):
        w_load((tp + k) % TP).start()

    loads[0].wait()
    pl.semaphore_wait(barrier, len(peers) + TP - 1)
    q_copies = [
        pltpu.make_async_remote_copy(
            qall.at[group], qall.at[group], q_send.at[i], q_recv.at[group],
            device_id={"group": peer}, device_id_type=MESH,
        )
        for i, peer in enumerate(peers)
    ]
    for copy in q_copies:
        copy.start()

    for h in range(HEADS):
        qf[h * ROWS : (h + 1) * ROWS, :] = qall[
            group, :, h * HEAD_DIM : (h + 1) * HEAD_DIM
        ].astype(jnp.float32)
    for copy in smalls:
        copy.wait()
    loads[1].wait()
    loads[2].wait()
    position = iota((HEADS, CAP), 1)
    for r in range(ROWS):
        pairs = pl.ds(r, HEADS, stride=ROWS)
        query = qf[pairs, :].astype(jnp.bfloat16)
        scores = dot_nt(query, ck[r]) * SCALE
        scores = jnp.where(position < lens[r], scores, FAR_BELOW)
        high = jnp.max(scores, axis=1, keepdims=True)
        weights = jnp.exp2(scores - high)
        local_high[pairs, :] = jnp.broadcast_to(high, (HEADS, HEAD_DIM))
        local_total[pairs, :] = jnp.broadcast_to(
            jnp.sum(weights, axis=1, keepdims=True), (HEADS, HEAD_DIM)
        )
        local_mixed[pairs, :] = dot(weights.astype(jnp.bfloat16), cv[r])

    def arrival(landing, sem, source):
        return pltpu.make_async_copy(landing.at[source], landing.at[source], sem.at[source])

    for peer in peers:
        arrival(qall, q_recv, peer).wait()
    pair = iota((SLOT_PAIRS, GROUPS * ROWS), 0)
    row = iota((SLOT_PAIRS, GROUPS * ROWS), 1)
    owned = jnp.where(pair < HEADS, owns[0], owns[1]) == row
    slot_query = jnp.zeros((SLOT_PAIRS, HEAD_DIM), jnp.float32)
    for h in range(HEADS):
        picked = jnp.where(owned & (pair % HEADS == h), 1.0, 0.0).astype(jnp.bfloat16)
        rows_of_head = qall[:, :, h * HEAD_DIM : (h + 1) * HEAD_DIM].reshape(GROUPS * ROWS, HEAD_DIM)
        slot_query += dot(picked, rows_of_head)
    slot_query = slot_query.astype(jnp.bfloat16)

    loads[3].wait()
    loads[4].wait()
    lane = iota((8, 128), 1)
    line = iota((8, 128), 0)
    base = (group % 8) * SLOT_PAIRS
    place = iota((HEADS, BLOCK), 1)
    table = jnp.zeros((8, 128), jnp.float32)
    for u in range(SLOTS):
        visible = place < fills[u]
        scores = dot_nt(slot_query[u * HEADS : (u + 1) * HEADS], pk[u]) * SCALE
        scores = jnp.where(visible, scores, FAR_BELOW)
        high = jnp.max(scores, axis=1, keepdims=True)
        weights = jnp.where(visible, jnp.exp2(scores - high), 0.0)
        total = jnp.sum(weights, axis=1, keepdims=True)
        mixed_all[group, u * HEADS : (u + 1) * HEADS, :] = dot(weights.astype(jnp.bfloat16), pv[u])
        own_lane = lane == base + u * HEADS + line
        high_line = jnp.sum(jnp.where(own_lane, high, 0.0), axis=0, keepdims=True)
        total_line = jnp.sum(jnp.where(own_lane, total, 0.0), axis=0, keepdims=True)
        in_slot = (lane >= base + u * HEADS) & (lane < base + (u + 1) * HEADS)
        owner = jnp.where(in_slot, owns[u].astype(jnp.float32), 0.0)
        table += jnp.where(line == 0, high_line, 0.0)
        table += jnp.where(line == 1, total_line, 0.0)
        table += jnp.where(line == 2, owner, 0.0)
    table += jnp.where((line == 3) & (lane == base), frees[0].astype(jnp.float32), 0.0)
    table_all[group] = table

    part_copies = []
    for i, peer in enumerate(peers):
        for landing, send, recv in ((mixed_all, m_send, m_recv), (table_all, t_send, t_recv)):
            copy = pltpu.make_async_remote_copy(
                landing.at[group], landing.at[group], send.at[i], recv.at[group],
                device_id={"group": peer}, device_id_type=MESH,
            )
            copy.start()
            part_copies.append(copy)
    for peer in peers:
        arrival(mixed_all, m_recv, peer).wait()
        arrival(table_all, t_recv, peer).wait()

    half = GROUPS // 2
    low = sum((table_all[g] for g in range(1, half)), table_all[0])
    top = sum((table_all[g] for g in range(half + 1, GROUPS)), table_all[half])
    table = jnp.concatenate([low, top], axis=1)
    free_ref[0] = jnp.sum(table[3:4, :]).astype(jnp.int32)
    span = (PAIRS, GROUPS * SLOT_PAIRS)
    own_pair = iota(span, 0)
    slot_pair = iota(span, 1)
    own_row = (own_pair % ROWS + group * ROWS).astype(jnp.float32)
    matched = (own_pair // ROWS == slot_pair % HEADS) & (table[2:3, :] == own_row)
    highs = jnp.where(matched, table[0:1, :], FAR_BELOW)
    far_high = jnp.max(highs, axis=1, keepdims=True)
    factor = jnp.where(matched, jnp.exp2(highs - far_high), 0.0)
    far_total = jnp.sum(factor * table[1:2, :], axis=1, keepdims=True)
    far_mixed = dot(
        factor, mixed_all[...].reshape(GROUPS * SLOT_PAIRS, HEAD_DIM), lax.Precision.HIGHEST
    )
    near_high = local_high[...]
    peak = jnp.maximum(near_high, far_high)
    near_scale = jnp.exp2(near_high - peak)
    far_scale = jnp.exp2(far_high - peak)
    attended = (near_scale * local_mixed[...] + far_scale * far_mixed) / (
        near_scale * local_total[...] + far_scale * far_total
    )
    attended = attended.astype(jnp.bfloat16)
    attended = jnp.concatenate(
        [attended[h * ROWS : (h + 1) * ROWS, :] for h in range(HEADS)], axis=1
    )

    def product_copy(block):
        return pltpu.make_async_remote_copy(
            sent.at[block], arrived.at[tp], o_send.at[block], o_recv.at[tp],
            device_id={"tp": block}, device_id_type=MESH,
        )

    def step(k, carry):
        block = (tp + k) % TP
        w_load(block).wait()
        sent[block] = dot(attended, w[block]).astype(jnp.bfloat16)
        product_copy(block).start()
        return carry

    lax.fori_loop(1, TP, step, 0)
    w_load(tp).wait()
    total = dot(attended, w[tp]).astype(jnp.bfloat16).astype(jnp.float32)
    for k in range(1, TP):
        source = (tp + k) % TP
        arrival(arrived, o_recv, source).wait()
        total += arrived[source].astype(jnp.float32)
    out_ref[...] = total.astype(jnp.bfloat16)

    for copy in q_copies + part_copies:
        copy.wait_send()
    for k in range(1, TP):
        product_copy((tp + k) % TP).wait_send()


def per_device(*args):
    bf16, f32 = jnp.bfloat16, jnp.float32
    dma = pltpu.SemaphoreType.DMA
    return pl.pallas_call(
        kernel,
        out_shape=(
            jax.ShapeDtypeStruct((ROWS, COLUMNS), bf16),
            jax.ShapeDtypeStruct((1,), jnp.int32),
        ),
        in_specs=[pl.BlockSpec(memory_space=pl.ANY)] * 10,
        out_specs=(
            pl.BlockSpec(memory_space=pltpu.VMEM),
            pl.BlockSpec(memory_space=pltpu.SMEM),
        ),
        scratch_shapes=[
            pltpu.VMEM((GROUPS, ROWS, WIDTH), bf16),
            pltpu.VMEM((ROWS, CAP, HEAD_DIM), bf16),
            pltpu.VMEM((ROWS, CAP, HEAD_DIM), bf16),
            pltpu.VMEM((SLOTS, BLOCK, HEAD_DIM), bf16),
            pltpu.VMEM((SLOTS, BLOCK, HEAD_DIM), bf16),
            pltpu.VMEM((TP, WIDTH, COLUMNS), bf16),
            pltpu.VMEM((PAIRS, HEAD_DIM), f32),
            pltpu.VMEM((PAIRS, HEAD_DIM), f32),
            pltpu.VMEM((PAIRS, HEAD_DIM), f32),
            pltpu.VMEM((PAIRS, HEAD_DIM), f32),
            pltpu.VMEM((GROUPS, SLOT_PAIRS, HEAD_DIM), f32),
            pltpu.VMEM((GROUPS, 8, 128), f32),
            pltpu.VMEM((TP, ROWS, COLUMNS), bf16),
            pltpu.VMEM((TP, ROWS, COLUMNS), bf16),
            pltpu.SMEM((ROWS,), jnp.int32),
            pltpu.SMEM((SLOTS,), jnp.int32),
            pltpu.SMEM((SLOTS,), jnp.int32),
            pltpu.SMEM((1,), jnp.int32),
            dma((5,)),
            dma((4,)),
            dma((TP,)),
            dma((GROUPS - 1,)),
            dma((GROUPS,)),
            dma((GROUPS - 1,)),
            dma((GROUPS,)),
            dma((GROUPS - 1,)),
            dma((GROUPS,)),
            dma((TP,)),
            dma((TP,)),
        ],
        compiler_params=pltpu.CompilerParams(
            collective_id=0, has_side_effects=True, vmem_limit_bytes=60 * 1024 * 1024
        ),
    )(*args)


def solution(mesh):
    in_specs = (
        P("group", "tp"),
        P("group", None, "tp"),
        P("group", None, "tp"),
        P("group", None, "tp"),
        P("group", None, "tp"),
        P("group"),
        P("group"),
        P("group"),
        P("group"),
        P("tp", None),
    )
    out_specs = (P("group", "tp"), P())
    return jax.shard_map(
        per_device, mesh=mesh, in_specs=in_specs, out_specs=out_specs, check_vma=False
    )
```

```python
import math

import jax
import jax.numpy as jnp
from jax import lax
from jax.experimental import pallas as pl
from jax.experimental.pallas import tpu as pltpu
from jax.sharding import PartitionSpec as P

MESH = pl.DeviceIdType.MESH
HEAD_DIM = 128
FAR_BELOW = -1e30
SCALE = math.log2(math.e) / math.sqrt(HEAD_DIM)

ROWS = 16
HEADS = 8
HALF_HEADS = 4
CAP = 512
SLOTS = 2
BLOCK = 4096
GROUPS = 16
TP = 8
WIDTH = HEADS * HEAD_DIM
COLUMNS = 1024
PAIRS = ROWS * HEADS
SLOT_PAIRS = SLOTS * HEADS

OFFSETS = sorted(
    ((dy, dx) for dy in range(4) for dx in range(4) if (dy, dx) != (0, 0)),
    key=lambda o: -(min(o[0], 4 - o[0]) + min(o[1], 4 - o[1])),
)


def dot_nt(a, b):
    return lax.dot_general(a, b, (((1,), (1,)), ((), ())), preferred_element_type=jnp.float32)


def dot(a, b, precision=None):
    return jnp.dot(a, b, preferred_element_type=jnp.float32, precision=precision)


def iota(shape, dim):
    return lax.broadcasted_iota(jnp.int32, shape, dim)


def kernel(
    q_hbm, ck_hbm, cv_hbm, pk_hbm, pv_hbm, len_hbm, own_hbm, fill_hbm, free_hbm, w_hbm,
    out_ref, free_ref,
    q_x, q_y, ask_x, ask_y, pick_x, pick_y, got_x, got_y,
    ck, cv, pk, pv, w, qf, scores_all, weights_all, near_high, near_total, near_mixed, joined,
    mixed_all, table_all, pair_sent, pair_got, z_sent, z_got,
    lens, owns, fills, frees,
    load_sem, small_sem, w_sem, q_send, q_recv, ask_send, ask_recv, pick_send, pick_recv,
    m_send, m_recv, t_send, t_recv, pair_send, pair_recv, z_send, z_recv,
):
    group = lax.axis_index("group")
    tp = lax.axis_index("tp")
    gy, gx = group // 4, group % 4
    z, core = tp // 2, tp % 2
    peers = [((gy + dy) % 4) * 4 + (gx + dx) % 4 for dy, dx in OFFSETS]
    steps = (2, 1, 3)

    def remote(src, dst, send, recv, **device):
        return pltpu.make_async_remote_copy(
            src, dst, send, recv, device_id=device, device_id_type=MESH
        )

    def arrival(landing, source, sem):
        pltpu.make_async_copy(landing.at[source], landing.at[source], sem).wait()

    half = WIDTH // 2
    loads = [
        pltpu.make_async_copy(src, dst, load_sem.at[i])
        for i, (src, dst) in enumerate(
            (
                (q_hbm.at[:, :half], q_x.at[gx]),
                (q_hbm.at[:, half:], q_y.at[gy]),
                (ck_hbm, ck),
                (cv_hbm, cv),
                (pk_hbm, pk),
                (pv_hbm, pv),
            )
        )
    ]
    smalls = [
        pltpu.make_async_copy(src, dst, small_sem.at[i])
        for i, (src, dst) in enumerate(
            ((own_hbm, owns), (len_hbm, lens), (fill_hbm, fills), (free_hbm, frees))
        )
    ]

    far_first = [(z + d) % 4 for d in (2, 1, 3, 0)]
    order = [2 * there + 1 - core for there in far_first] + [2 * there + core for there in far_first]

    def w_load(block):
        columns = pl.ds(pl.multiple_of(block * COLUMNS, COLUMNS), COLUMNS)
        return pltpu.make_async_copy(w_hbm.at[:, columns], w.at[block], w_sem.at[block])

    loads[0].start()
    loads[1].start()
    smalls[0].start()
    barrier = pltpu.get_barrier_semaphore()
    for d in steps:
        pl.semaphore_signal(
            barrier, inc=1, device_id={"group": gy * 4 + (gx + d) % 4}, device_id_type=MESH
        )
        pl.semaphore_signal(
            barrier, inc=1, device_id={"group": (gy + d) % 4 * 4 + gx}, device_id_type=MESH
        )
        pl.semaphore_signal(
            barrier, inc=1, device_id={"tp": (z + d) % 4 * 2 + core}, device_id_type=MESH
        )
    pl.semaphore_signal(barrier, inc=1, device_id={"tp": 2 * z + 1 - core}, device_id_type=MESH)
    for copy in loads[2:] + smalls[1:]:
        copy.start()

    smalls[0].wait()
    asked = jnp.where(iota((8, 128), 0) < HALF_HEADS, owns[0], owns[1])
    asked = asked.astype(jnp.float32).astype(jnp.bfloat16)
    ask_x[gx] = asked
    ask_y[gy] = asked
    loads[0].wait()
    loads[1].wait()
    pl.semaphore_wait(barrier, 3 * len(steps) + 1)
    started = []
    for i, d in enumerate(steps):
        along_x, along_y = gy * 4 + (gx + d) % 4, (gy + d) % 4 * 4 + gx
        started += [
            remote(q_x.at[gx], q_x.at[gx], q_send.at[0, i], q_recv.at[0, gx], group=along_x),
            remote(ask_x.at[gx], ask_x.at[gx], ask_send.at[0, i], ask_recv.at[0, gx], group=along_x),
            remote(q_y.at[gy], q_y.at[gy], q_send.at[1, i], q_recv.at[1, gy], group=along_y),
            remote(ask_y.at[gy], ask_y.at[gy], ask_send.at[1, i], ask_recv.at[1, gy], group=along_y),
        ]
    for copy in started:
        copy.start()
    for block in order:
        w_load(block).start()

    for h in range(HALF_HEADS):
        lanes = slice(h * HEAD_DIM, (h + 1) * HEAD_DIM)
        qf[h * ROWS : (h + 1) * ROWS, :] = q_x[gx, :, lanes].astype(jnp.float32)
        other = h + HALF_HEADS
        qf[other * ROWS : (other + 1) * ROWS, :] = q_y[gy, :, lanes].astype(jnp.float32)
    loads[2].wait()
    for r in range(ROWS):
        query = qf[pl.ds(r, HEADS, stride=ROWS), :].astype(jnp.bfloat16)
        scores_all[r] = dot_nt(query, ck[r])

    for d in steps:
        other_x, other_y = (gx + d) % 4, (gy + d) % 4
        arrival(ask_x, other_x, ask_recv.at[0, other_x])
        arrival(ask_y, other_y, ask_recv.at[1, other_y])
        arrival(q_x, other_x, q_recv.at[0, other_x])
        arrival(q_y, other_y, q_recv.at[1, other_y])

    rows_here = 4 * ROWS
    shape = (4 * 8, rows_here)
    head_of = iota(shape, 0) % HALF_HEADS
    lane = iota(shape, 1)

    def picked(asks, queries, row_of_lane):
        wanted = asks[...].reshape(4 * 8, 128)[:, :rows_here].astype(jnp.float32)
        match = wanted == row_of_lane.astype(jnp.float32)
        found = jnp.zeros((4 * 8, HEAD_DIM), jnp.float32)
        for h in range(HALF_HEADS):
            chosen = jnp.where(match & (head_of == h), 1.0, 0.0).astype(jnp.bfloat16)
            rows = queries[:, :, h * HEAD_DIM : (h + 1) * HEAD_DIM].reshape(rows_here, HEAD_DIM)
            found += dot(chosen, rows)
        return found.astype(jnp.bfloat16).reshape(4, 8, HEAD_DIM)

    pick_x[...] = picked(ask_y, q_x, lane + gy * rows_here)
    pick_y[...] = picked(ask_x, q_y, lane // ROWS * rows_here + lane % ROWS + gx * ROWS)
    for i, d in enumerate(steps):
        other_x, other_y = (gx + d) % 4, (gy + d) % 4
        for copy in (
            remote(
                pick_x.at[other_y], got_x.at[gy], pick_send.at[0, i], pick_recv.at[0, gy],
                group=other_y * 4 + gx,
            ),
            remote(
                pick_y.at[other_x], got_y.at[gx], pick_send.at[1, i], pick_recv.at[1, gx],
                group=gy * 4 + other_x,
            ),
        ):
            copy.start()
            started.append(copy)
    got_x[gy] = pick_x[gy]
    got_y[gx] = pick_y[gx]

    for copy in smalls[1:]:
        copy.wait()
    position = iota((HEADS, CAP), 1)
    for r in range(ROWS):
        pairs = slice(r * HEADS, (r + 1) * HEADS)
        scores = jnp.where(position < lens[r], scores_all[r] * SCALE, FAR_BELOW)
        high = jnp.max(scores, axis=1, keepdims=True)
        weights = jnp.exp2(scores - high)
        total = jnp.sum(weights, axis=1, keepdims=True)
        near_high[pairs, :] = jnp.broadcast_to(high, (HEADS, HEAD_DIM))
        near_total[pairs, :] = jnp.broadcast_to(total, (HEADS, HEAD_DIM))
        weights_all[r] = weights.astype(jnp.bfloat16)
    loads[3].wait()
    for r in range(ROWS):
        near_mixed[r * HEADS : (r + 1) * HEADS, :] = dot(weights_all[r], cv[r])
    loads[4].wait()
    loads[5].wait()

    for d in steps:
        other_x, other_y = (gx + d) % 4, (gy + d) % 4
        arrival(got_x, other_y, pick_recv.at[0, other_y])
        arrival(got_y, other_x, pick_recv.at[1, other_x])

    first = jnp.sum(got_x[...].astype(jnp.float32), axis=0)
    last = jnp.sum(got_y[...].astype(jnp.float32), axis=0)
    lane = iota((8, 128), 1)
    line = iota((8, 128), 0)
    base = (group % 8) * SLOT_PAIRS
    place = iota((HEADS, BLOCK), 1)
    table = jnp.zeros((8, 128), jnp.float32)
    slot_mixed = []
    for u in range(SLOTS):
        heads = slice(u * HALF_HEADS, (u + 1) * HALF_HEADS)
        query = jnp.concatenate([first[heads], last[heads]], axis=0).astype(jnp.bfloat16)
        visible = place < fills[u]
        scores = jnp.where(visible, dot_nt(query, pk[u]) * SCALE, FAR_BELOW)
        high = jnp.max(scores, axis=1, keepdims=True)
        weights = jnp.where(visible, jnp.exp2(scores - high), 0.0)
        total = jnp.sum(weights, axis=1, keepdims=True)
        slot_mixed.append(dot(weights.astype(jnp.bfloat16), pv[u]))
        own_lane = lane == base + u * HEADS + line
        high_line = jnp.sum(jnp.where(own_lane, high, 0.0), axis=0, keepdims=True)
        total_line = jnp.sum(jnp.where(own_lane, total, 0.0), axis=0, keepdims=True)
        in_slot = (lane >= base + u * HEADS) & (lane < base + (u + 1) * HEADS)
        owner = jnp.where(in_slot, owns[u].astype(jnp.float32), 0.0)
        table += jnp.where(line == 0, high_line, 0.0)
        table += jnp.where(line == 1, total_line, 0.0)
        table += jnp.where(line == 2, owner, 0.0)
    table += jnp.where((line == 3) & (lane == base), frees[0].astype(jnp.float32), 0.0)
    table_all[group] = table
    mixed_all[group] = jnp.concatenate(slot_mixed, axis=0).astype(jnp.bfloat16)

    for i, peer in enumerate(peers):
        for copy in (
            remote(
                mixed_all.at[group], mixed_all.at[group], m_send.at[i], m_recv.at[group], group=peer
            ),
            remote(
                table_all.at[group], table_all.at[group], t_send.at[i], t_recv.at[group], group=peer
            ),
        ):
            copy.start()
            started.append(copy)
    for peer in peers:
        arrival(table_all, peer, t_recv.at[peer])
        arrival(mixed_all, peer, m_recv.at[peer])

    middle = GROUPS // 2
    low = sum((table_all[g] for g in range(1, middle)), table_all[0])
    top = sum((table_all[g] for g in range(middle + 1, GROUPS)), table_all[middle])
    table = jnp.concatenate([low, top], axis=1)
    free_ref[0] = jnp.sum(table[3:4, :]).astype(jnp.int32)
    span = (PAIRS, GROUPS * SLOT_PAIRS)
    own_pair = iota(span, 0)
    slot_pair = iota(span, 1)
    own_row = (own_pair // HEADS + group * ROWS).astype(jnp.float32)
    matched = (own_pair % HEADS == slot_pair % HEADS) & (table[2:3, :] == own_row)
    highs = jnp.where(matched, table[0:1, :], FAR_BELOW)
    far_high = jnp.max(highs, axis=1, keepdims=True)
    factor = jnp.where(matched, jnp.exp2(highs - far_high), 0.0)
    far_total = jnp.sum(factor * table[1:2, :], axis=1, keepdims=True)
    coarse = factor.astype(jnp.bfloat16)
    fine = (factor - coarse.astype(jnp.float32)).astype(jnp.bfloat16)
    parts = mixed_all[...].reshape(GROUPS * SLOT_PAIRS, HEAD_DIM)
    far_mixed = dot(coarse, parts) + dot(fine, parts)
    near = near_high[...]
    peak = jnp.maximum(near, far_high)
    near_scale = jnp.exp2(near - peak)
    far_scale = jnp.exp2(far_high - peak)
    joined[...] = (near_scale * near_mixed[...] + far_scale * far_mixed) / (
        near_scale * near_total[...] + far_scale * far_total
    )
    attended = jnp.concatenate(
        [joined[pl.ds(h, ROWS, stride=HEADS), :].astype(jnp.bfloat16) for h in range(HEADS)], axis=1
    )

    for i, there in enumerate(far_first):
        block = order[i]
        w_load(block).wait()
        pair_sent[there] = dot(attended, w[block])
        copy = remote(
            pair_sent.at[there], pair_got.at[there], pair_send.at[i], pair_recv.at[there],
            tp=2 * z + 1 - core,
        )
        copy.start()
        started.append(copy)
    for i, there in enumerate(far_first):
        block = order[4 + i]
        w_load(block).wait()
        product = dot(attended, w[block])
        arrival(pair_got, there, pair_recv.at[there])
        product += pair_got[there]
        if i < 3:
            z_sent[there] = product.astype(jnp.bfloat16)
            copy = remote(
                z_sent.at[there], z_got.at[z], z_send.at[i], z_recv.at[z], tp=2 * there + core
            )
            copy.start()
            started.append(copy)
    for d in (1, 3, 2):
        source = (z + d) % 4
        arrival(z_got, source, z_recv.at[source])
        product += z_got[source].astype(jnp.float32)
    out_ref[...] = product.astype(jnp.bfloat16)

    for copy in started:
        copy.wait_send()


def per_device(*args):
    bf16, f32 = jnp.bfloat16, jnp.float32
    dma = pltpu.SemaphoreType.DMA
    return pl.pallas_call(
        kernel,
        out_shape=(
            jax.ShapeDtypeStruct((ROWS, COLUMNS), bf16),
            jax.ShapeDtypeStruct((1,), jnp.int32),
        ),
        in_specs=[pl.BlockSpec(memory_space=pltpu.HBM)] * 10,
        out_specs=(
            pl.BlockSpec(memory_space=pltpu.VMEM),
            pl.BlockSpec(memory_space=pltpu.SMEM),
        ),
        scratch_shapes=[
            pltpu.VMEM((4, ROWS, WIDTH // 2), bf16),
            pltpu.VMEM((4, ROWS, WIDTH // 2), bf16),
            pltpu.VMEM((4, 8, 128), bf16),
            pltpu.VMEM((4, 8, 128), bf16),
            pltpu.VMEM((4, 8, HEAD_DIM), bf16),
            pltpu.VMEM((4, 8, HEAD_DIM), bf16),
            pltpu.VMEM((4, 8, HEAD_DIM), bf16),
            pltpu.VMEM((4, 8, HEAD_DIM), bf16),
            pltpu.VMEM((ROWS, CAP, HEAD_DIM), bf16),
            pltpu.VMEM((ROWS, CAP, HEAD_DIM), bf16),
            pltpu.VMEM((SLOTS, BLOCK, HEAD_DIM), bf16),
            pltpu.VMEM((SLOTS, BLOCK, HEAD_DIM), bf16),
            pltpu.VMEM((TP, WIDTH, COLUMNS), bf16),
            pltpu.VMEM((PAIRS, HEAD_DIM), f32),
            pltpu.VMEM((ROWS, HEADS, CAP), f32),
            pltpu.VMEM((ROWS, HEADS, CAP), bf16),
            pltpu.VMEM((PAIRS, HEAD_DIM), f32),
            pltpu.VMEM((PAIRS, HEAD_DIM), f32),
            pltpu.VMEM((PAIRS, HEAD_DIM), f32),
            pltpu.VMEM((PAIRS, HEAD_DIM), f32),
            pltpu.VMEM((GROUPS, SLOT_PAIRS, HEAD_DIM), bf16),
            pltpu.VMEM((GROUPS, 8, 128), f32),
            pltpu.VMEM((4, ROWS, COLUMNS), f32),
            pltpu.VMEM((4, ROWS, COLUMNS), f32),
            pltpu.VMEM((4, ROWS, COLUMNS), bf16),
            pltpu.VMEM((4, ROWS, COLUMNS), bf16),
            pltpu.SMEM((ROWS,), jnp.int32),
            pltpu.SMEM((SLOTS,), jnp.int32),
            pltpu.SMEM((SLOTS,), jnp.int32),
            pltpu.SMEM((1,), jnp.int32),
            dma((6,)),
            dma((4,)),
            dma((TP,)),
            dma((2, 3)),
            dma((2, 4)),
            dma((2, 3)),
            dma((2, 4)),
            dma((2, 3)),
            dma((2, 4)),
            dma((GROUPS - 1,)),
            dma((GROUPS,)),
            dma((GROUPS - 1,)),
            dma((GROUPS,)),
            dma((4,)),
            dma((4,)),
            dma((3,)),
            dma((4,)),
        ],
        compiler_params=pltpu.CompilerParams(
            collective_id=0, has_side_effects=True, vmem_limit_bytes=60 * 1024 * 1024
        ),
    )(*args)


def solution(mesh):
    in_specs = (
        P("group", "tp"),
        P("group", None, "tp"),
        P("group", None, "tp"),
        P("group", None, "tp"),
        P("group", None, "tp"),
        P("group"),
        P("group"),
        P("group"),
        P("group"),
        P("tp", None),
    )
    out_specs = (P("group", "tp"), P())
    return jax.shard_map(
        per_device, mesh=mesh, in_specs=in_specs, out_specs=out_specs, check_vma=False
    )
```

```python
import math

import jax
import jax.numpy as jnp
from jax import lax
from jax.experimental import pallas as pl
from jax.experimental.pallas import tpu as pltpu
from jax.sharding import PartitionSpec as P

MESH = pl.DeviceIdType.MESH
HEAD_DIM = 128
FAR_BELOW = -1e30
SCALE = math.log2(math.e) / math.sqrt(HEAD_DIM)

ROWS = 16
HEADS = 8
HALF_HEADS = 4
CAP = 512
SLOTS = 2
BLOCK = 4096
GROUPS = 16
TP = 8
WIDTH = HEADS * HEAD_DIM
COLUMNS = 1024
PAIRS = ROWS * HEADS
SLOT_PAIRS = SLOTS * HEADS

OFFSETS = sorted(
    ((dy, dx) for dy in range(4) for dx in range(4) if (dy, dx) != (0, 0)),
    key=lambda o: -(min(o[0], 4 - o[0]) + min(o[1], 4 - o[1])),
)


def dot_nt(a, b):
    return lax.dot_general(a, b, (((1,), (1,)), ((), ())), preferred_element_type=jnp.float32)


def dot(a, b, precision=None):
    return jnp.dot(a, b, preferred_element_type=jnp.float32, precision=precision)


def iota(shape, dim):
    return lax.broadcasted_iota(jnp.int32, shape, dim)


def kernel(
    q_hbm, ck_hbm, cv_hbm, pk_hbm, pv_hbm, len_hbm, own_hbm, fill_hbm, free_hbm, w_hbm,
    out_ref, free_ref,
    q_x, q_y, ask_x, ask_y, pick_x, pick_y, got_x, got_y,
    ck, cv, pk, pv, w, qf, scores_all, weights_all, near_high, near_total, near_mixed, joined,
    mixed_all, table_all, known_all, pair_sent, pair_got, z_sent, z_got,
    lens, owns, fills, frees,
    q_load, k_load, v_load, pool_load, small_load, w_load, send_sem, query_sem, pick_sem, part_sem,
    pair_sem, z_sem,
):
    group = lax.axis_index("group")
    tp = lax.axis_index("tp")
    gy, gx = group // 4, group % 4
    z, core = tp // 2, tp % 2
    peers = [((gy + dy) % 4) * 4 + (gx + dx) % 4 for dy, dx in OFFSETS]
    steps = (2, 1, 3)

    def remote(src, dst, arrived, **device):
        return pltpu.make_async_remote_copy(
            src, dst, send_sem, arrived, device_id=device, device_id_type=MESH
        )

    def wait_bytes(kib, sem):
        lines = pv.at[0, pl.ds(0, kib * 4)]
        pltpu.make_async_copy(lines, lines, sem).wait()

    half = WIDTH // 2
    loads = [
        pltpu.make_async_copy(q_hbm.at[:, :half], q_x.at[gx], q_load),
        pltpu.make_async_copy(q_hbm.at[:, half:], q_y.at[gy], q_load),
        pltpu.make_async_copy(ck_hbm, ck, k_load),
        pltpu.make_async_copy(cv_hbm, cv, v_load),
        pltpu.make_async_copy(pk_hbm, pk, pool_load),
        pltpu.make_async_copy(pv_hbm, pv, pool_load),
    ]
    smalls = [
        pltpu.make_async_copy(src, dst, small_load.at[i])
        for i, (src, dst) in enumerate(
            ((own_hbm, owns), (len_hbm, lens), (fill_hbm, fills), (free_hbm, frees))
        )
    ]

    far_first = [(z + d) % 4 for d in (2, 1, 3, 0)]
    turns = [(0, 0), (0, 1), (0, 2), (1, 0), (1, 1), (1, 2), (0, 3), (1, 3)]
    order = [2 * far_first[i] + (core if own else 1 - core) for own, i in turns]

    def w_copy(block):
        columns = pl.ds(pl.multiple_of(block * COLUMNS, COLUMNS), COLUMNS)
        return pltpu.make_async_copy(w_hbm.at[:, columns], w.at[block], w_load)

    loads[0].start()
    loads[1].start()
    smalls[0].start()
    barrier = pltpu.get_barrier_semaphore()
    for d in steps:
        pl.semaphore_signal(
            barrier, inc=1, device_id={"group": gy * 4 + (gx + d) % 4}, device_id_type=MESH
        )
        pl.semaphore_signal(
            barrier, inc=1, device_id={"group": (gy + d) % 4 * 4 + gx}, device_id_type=MESH
        )
        pl.semaphore_signal(
            barrier, inc=1, device_id={"tp": (z + d) % 4 * 2 + core}, device_id_type=MESH
        )
    pl.semaphore_signal(barrier, inc=1, device_id={"tp": 2 * z + 1 - core}, device_id_type=MESH)
    for copy in loads[2:] + smalls[1:]:
        copy.start()

    smalls[0].wait()
    asked = jnp.where(iota((8, 128), 0) < HALF_HEADS, owns[0], owns[1])
    asked = asked.astype(jnp.float32).astype(jnp.bfloat16)
    ask_x[gx] = asked
    ask_y[gy] = asked
    pltpu.make_async_copy(q_x.at[0:2], q_x.at[0:2], q_load).wait()
    pl.semaphore_wait(barrier, 3 * len(steps) + 1)
    started = []
    for d in steps:
        along_x, along_y = gy * 4 + (gx + d) % 4, (gy + d) % 4 * 4 + gx
        started += [
            remote(ask_x.at[gx], ask_x.at[gx], query_sem, group=along_x),
            remote(ask_y.at[gy], ask_y.at[gy], query_sem, group=along_y),
            remote(q_x.at[gx], q_x.at[gx], query_sem, group=along_x),
            remote(q_y.at[gy], q_y.at[gy], query_sem, group=along_y),
        ]
    for copy in started:
        copy.start()
    for block in order:
        w_copy(block).start()

    for h in range(HALF_HEADS):
        lanes = slice(h * HEAD_DIM, (h + 1) * HEAD_DIM)
        qf[h * ROWS : (h + 1) * ROWS, :] = q_x[gx, :, lanes].astype(jnp.float32)
        other = h + HALF_HEADS
        qf[other * ROWS : (other + 1) * ROWS, :] = q_y[gy, :, lanes].astype(jnp.float32)
    loads[2].wait()
    for r in range(ROWS):
        query = qf[pl.ds(r, HEADS, stride=ROWS), :].astype(jnp.bfloat16)
        scores_all[r] = dot_nt(query, ck[r])

    wait_bytes(2 * 3 * (16 + 2), query_sem)

    rows_here = 4 * ROWS
    shape = (4 * 8, rows_here)
    head_of = iota(shape, 0) % HALF_HEADS
    lane = iota(shape, 1)

    def picked(asks, queries, row_of_lane):
        wanted = asks[...].reshape(4 * 8, 128)[:, :rows_here].astype(jnp.float32)
        match = wanted == row_of_lane.astype(jnp.float32)
        found = jnp.zeros((4 * 8, HEAD_DIM), jnp.float32)
        for h in range(HALF_HEADS):
            chosen = jnp.where(match & (head_of == h), 1.0, 0.0).astype(jnp.bfloat16)
            rows = queries[:, :, h * HEAD_DIM : (h + 1) * HEAD_DIM].reshape(rows_here, HEAD_DIM)
            found += dot(chosen, rows)
        return found.astype(jnp.bfloat16).reshape(4, 8, HEAD_DIM)

    pick_x[...] = picked(ask_y, q_x, lane + gy * rows_here)
    pick_y[...] = picked(ask_x, q_y, lane // ROWS * rows_here + lane % ROWS + gx * ROWS)
    for d in steps:
        other_x, other_y = (gx + d) % 4, (gy + d) % 4
        remote(pick_x.at[other_y], got_x.at[gy], pick_sem, group=other_y * 4 + gx).start()
        remote(pick_y.at[other_x], got_y.at[gx], pick_sem, group=gy * 4 + other_x).start()
    got_x[gy] = pick_x[gy]
    got_y[gx] = pick_y[gx]


    for copy in smalls[1:]:
        copy.wait()
    line = iota((2, 128), 0)
    lane = iota((2, 128), 1)
    base = (group % 8) * SLOT_PAIRS
    known = jnp.where((line == 1) & (lane == base), frees[0].astype(jnp.float32), 0.0)
    for u in range(SLOTS):
        in_slot = (lane >= base + u * HEADS) & (lane < base + (u + 1) * HEADS)
        known += jnp.where((line == 0) & in_slot, owns[u].astype(jnp.float32), 0.0)
    known_all[group] = known
    for peer in peers:
        remote(known_all.at[group], known_all.at[group], part_sem, group=peer).start()

    position = iota((HEADS, CAP), 1)
    for r in range(ROWS):
        pairs = slice(r * HEADS, (r + 1) * HEADS)
        scores = jnp.where(position < lens[r], scores_all[r] * SCALE, FAR_BELOW)
        high = jnp.max(scores, axis=1, keepdims=True)
        weights = jnp.exp2(scores - high)
        total = jnp.sum(weights, axis=1, keepdims=True)
        near_high[pairs, :] = jnp.broadcast_to(high, (HEADS, HEAD_DIM))
        near_total[pairs, :] = jnp.broadcast_to(total, (HEADS, HEAD_DIM))
        weights_all[r] = weights.astype(jnp.bfloat16)
    loads[3].wait()
    for r in range(ROWS):
        near_mixed[r * HEADS : (r + 1) * HEADS, :] = dot(weights_all[r], cv[r])
    pltpu.make_async_copy(w.at[0:2], w.at[0:2], pool_load).wait()

    wait_bytes(2 * 3 * 2, pick_sem)

    first = jnp.sum(got_x[...].astype(jnp.float32), axis=0)
    last = jnp.sum(got_y[...].astype(jnp.float32), axis=0)
    lane = iota((8, 128), 1)
    line = iota((8, 128), 0)
    place = iota((HEADS, BLOCK), 1)
    highs, totals = jnp.zeros((1, 128), jnp.float32), jnp.zeros((1, 128), jnp.float32)
    slot_mixed = []
    for u in range(SLOTS):
        heads = slice(u * HALF_HEADS, (u + 1) * HALF_HEADS)
        query = jnp.concatenate([first[heads], last[heads]], axis=0).astype(jnp.bfloat16)
        visible = place < fills[u]
        scores = jnp.where(visible, dot_nt(query, pk[u]) * SCALE, FAR_BELOW)
        high = jnp.max(scores, axis=1, keepdims=True)
        weights = jnp.where(visible, jnp.exp2(scores - high), 0.0)
        total = jnp.sum(weights, axis=1, keepdims=True)
        slot_mixed.append(dot(weights.astype(jnp.bfloat16), pv[u]))
        own_lane = lane == base + u * HEADS + line
        highs += jnp.sum(jnp.where(own_lane, high, 0.0), axis=0, keepdims=True)
        totals += jnp.sum(jnp.where(own_lane, total, 0.0), axis=0, keepdims=True)
    table_all[group] = jnp.concatenate([highs, totals], axis=0)
    mixed_all[group] = jnp.concatenate(slot_mixed, axis=0).astype(jnp.bfloat16)

    for peer in peers:
        remote(mixed_all.at[group], mixed_all.at[group], part_sem, group=peer).start()
        remote(table_all.at[group], table_all.at[group], part_sem, group=peer).start()
    wait_bytes(len(peers) * (4 + 1 + 1), part_sem)

    middle = GROUPS // 2

    def joint(tables):
        low = sum((tables[g] for g in range(1, middle)), tables[0])
        top = sum((tables[g] for g in range(middle + 1, GROUPS)), tables[middle])
        return jnp.concatenate([low, top], axis=1)

    table, known = joint(table_all), joint(known_all)
    free_total = jnp.sum(known[1:2, :], axis=1, keepdims=True).astype(jnp.int32)
    free_ref[...] = jnp.broadcast_to(free_total, (8, 128))
    span = (PAIRS, GROUPS * SLOT_PAIRS)
    own_pair = iota(span, 0)
    slot_pair = iota(span, 1)
    own_row = (own_pair // HEADS + group * ROWS).astype(jnp.float32)
    matched = (own_pair % HEADS == slot_pair % HEADS) & (known[0:1, :] == own_row)
    highs = jnp.where(matched, table[0:1, :], FAR_BELOW)
    far_high = jnp.max(highs, axis=1, keepdims=True)
    factor = jnp.where(matched, jnp.exp2(highs - far_high), 0.0)
    far_total = jnp.sum(factor * table[1:2, :], axis=1, keepdims=True)
    coarse = factor.astype(jnp.bfloat16)
    fine = (factor - coarse.astype(jnp.float32)).astype(jnp.bfloat16)
    parts = mixed_all[...].reshape(GROUPS * SLOT_PAIRS, HEAD_DIM)
    far_mixed = dot(coarse, parts) + dot(fine, parts)
    near = near_high[...]
    peak = jnp.maximum(near, far_high)
    near_scale = jnp.exp2(near - peak)
    far_scale = jnp.exp2(far_high - peak)
    joined[...] = (near_scale * near_mixed[...] + far_scale * far_mixed) / (
        near_scale * near_total[...] + far_scale * far_total
    )
    attended = jnp.concatenate(
        [joined[pl.ds(h, ROWS, stride=HEADS), :].astype(jnp.bfloat16) for h in range(HEADS)], axis=1
    )

    pltpu.make_async_copy(w, w, w_load).wait()
    for block, (own, i) in zip(order, turns):
        there = far_first[i]
        product = dot(attended, w[block])
        if not own:
            pair_sent[there] = product
            remote(
                pair_sent.at[there], pair_got.at[there], pair_sem.at[there], tp=2 * z + 1 - core
            ).start()
            continue
        pltpu.make_async_copy(pair_got.at[there], pair_got.at[there], pair_sem.at[there]).wait()
        product += pair_got[there]
        if i < 3:
            z_sent[there] = product.astype(jnp.bfloat16)
            remote(z_sent.at[there], z_got.at[z], z_sem, tp=2 * there + core).start()
    wait_bytes(3 * 32, z_sem)
    for d in (1, 3, 2):
        product += z_got[(z + d) % 4].astype(jnp.float32)
    out_ref[...] = product

    wait_bytes(96 + 12 + 12 + 90 + 256 + 96, send_sem)


def finish(summed, free, out_ref, free_ref):
    out_ref[...] = summed[...].astype(jnp.bfloat16)
    free_ref[0] = free[0, 0]


def per_device(*args):
    bf16, f32 = jnp.bfloat16, jnp.float32
    dma = pltpu.SemaphoreType.DMA
    summed, free = pl.pallas_call(
        kernel,
        out_shape=(
            pltpu.VMEM((ROWS, COLUMNS), f32),
            pltpu.VMEM((8, 128), jnp.int32),
        ),
        in_specs=[pl.BlockSpec(memory_space=pltpu.HBM)] * 10,
        out_specs=(
            pl.BlockSpec(memory_space=pltpu.VMEM),
            pl.BlockSpec(memory_space=pltpu.VMEM),
        ),
        scratch_shapes=[
            pltpu.VMEM((4, ROWS, WIDTH // 2), bf16),
            pltpu.VMEM((4, ROWS, WIDTH // 2), bf16),
            pltpu.VMEM((4, 8, 128), bf16),
            pltpu.VMEM((4, 8, 128), bf16),
            pltpu.VMEM((4, 8, HEAD_DIM), bf16),
            pltpu.VMEM((4, 8, HEAD_DIM), bf16),
            pltpu.VMEM((4, 8, HEAD_DIM), bf16),
            pltpu.VMEM((4, 8, HEAD_DIM), bf16),
            pltpu.VMEM((ROWS, CAP, HEAD_DIM), bf16),
            pltpu.VMEM((ROWS, CAP, HEAD_DIM), bf16),
            pltpu.VMEM((SLOTS, BLOCK, HEAD_DIM), bf16),
            pltpu.VMEM((SLOTS, BLOCK, HEAD_DIM), bf16),
            pltpu.VMEM((TP, WIDTH, COLUMNS), bf16),
            pltpu.VMEM((PAIRS, HEAD_DIM), f32),
            pltpu.VMEM((ROWS, HEADS, CAP), f32),
            pltpu.VMEM((ROWS, HEADS, CAP), bf16),
            pltpu.VMEM((PAIRS, HEAD_DIM), f32),
            pltpu.VMEM((PAIRS, HEAD_DIM), f32),
            pltpu.VMEM((PAIRS, HEAD_DIM), f32),
            pltpu.VMEM((PAIRS, HEAD_DIM), f32),
            pltpu.VMEM((GROUPS, SLOT_PAIRS, HEAD_DIM), bf16),
            pltpu.VMEM((GROUPS, 2, 128), f32),
            pltpu.VMEM((GROUPS, 2, 128), f32),
            pltpu.VMEM((4, ROWS, COLUMNS), f32),
            pltpu.VMEM((4, ROWS, COLUMNS), f32),
            pltpu.VMEM((4, ROWS, COLUMNS), bf16),
            pltpu.VMEM((4, ROWS, COLUMNS), bf16),
            pltpu.SMEM((ROWS,), jnp.int32),
            pltpu.SMEM((SLOTS,), jnp.int32),
            pltpu.SMEM((SLOTS,), jnp.int32),
            pltpu.SMEM((1,), jnp.int32),
            dma,
            dma,
            dma,
            dma,
            dma((4,)),
            dma,
            dma,
            dma,
            dma,
            dma,
            dma((4,)),
            dma,
        ],
        compiler_params=pltpu.CompilerParams(
            collective_id=0, has_side_effects=True, vmem_limit_bytes=60 * 1024 * 1024
        ),
    )(*args)
    return pl.pallas_call(
        finish,
        out_shape=(
            jax.ShapeDtypeStruct((ROWS, COLUMNS), bf16),
            jax.ShapeDtypeStruct((1,), jnp.int32),
        ),
        in_specs=[pl.BlockSpec(memory_space=pltpu.VMEM)] * 2,
        out_specs=(
            pl.BlockSpec(memory_space=pltpu.VMEM),
            pl.BlockSpec(memory_space=pltpu.SMEM),
        ),
        compiler_params=pltpu.CompilerParams(vmem_limit_bytes=1024 * 1024),
    )(
        pltpu.with_memory_space_constraint(summed, pltpu.VMEM),
        pltpu.with_memory_space_constraint(free, pltpu.VMEM),
    )


def solution(mesh):
    in_specs = (
        P("group", "tp"),
        P("group", None, "tp"),
        P("group", None, "tp"),
        P("group", None, "tp"),
        P("group", None, "tp"),
        P("group"),
        P("group"),
        P("group"),
        P("group"),
        P("tp", None),
    )
    out_specs = (P("group", "tp"), P())
    return jax.shard_map(
        per_device, mesh=mesh, in_specs=in_specs, out_specs=out_specs, check_vma=False
    )
```

```python
import math

import jax
import jax.numpy as jnp
from jax import lax
from jax.experimental import pallas as pl
from jax.experimental.pallas import tpu as pltpu
from jax.sharding import PartitionSpec as P

MESH = pl.DeviceIdType.MESH
HEAD_DIM = 128
FAR_BELOW = -1e30
SCALE = math.log2(math.e) / math.sqrt(HEAD_DIM)

ROWS = 16
HEADS = 8
HALF_HEADS = 4
UNUSED, LANDED = 8, 9
CAP = 512
SLOTS = 2
BLOCK = 4096
GROUPS = 16
TP = 8
WIDTH = HEADS * HEAD_DIM
COLUMNS = 1024
PAIRS = ROWS * HEADS
SLOT_PAIRS = SLOTS * HEADS

OFFSETS = sorted(
    ((dy, dx) for dy in range(4) for dx in range(4) if (dy, dx) != (0, 0)),
    key=lambda o: -(min(o[0], 4 - o[0]) + min(o[1], 4 - o[1])),
)


def dot_nt(a, b):
    return lax.dot_general(a, b, (((1,), (1,)), ((), ())), preferred_element_type=jnp.float32)


def dot(a, b, precision=None):
    return jnp.dot(a, b, preferred_element_type=jnp.float32, precision=precision)


def iota(shape, dim):
    return lax.broadcasted_iota(jnp.int32, shape, dim)


def kernel(
    q_hbm, ck_hbm, cv_hbm, pk_hbm, pv_hbm, len_hbm, own_hbm, fill_hbm, free_hbm, w_hbm,
    out_ref, free_ref,
    q_x, q_y, ask_x, ask_y, pick_x, pick_y, got_x, got_y,
    ck, cv, pk, pv, w, qf, scores_all, weights_all, near_high, near_total, near_mixed, joined, attended_all,
    mixed_all, table_all, known_all, sent, got,
    lens, owns, fills, frees,
    q_load, k_load, v_load, pool_load, small_load, w_load, send_sem, query_sem, pick_sem, part_sem,
    got_sem,
):
    group = lax.axis_index("group")
    tp = lax.axis_index("tp")
    gy, gx = group // 4, group % 4
    z, core = tp // 2, tp % 2
    peers = [((gy + dy) % 4) * 4 + (gx + dx) % 4 for dy, dx in OFFSETS]
    steps = (2, 1, 3)

    def remote(src, dst, arrived, **device):
        return pltpu.make_async_remote_copy(
            src, dst, send_sem, arrived, device_id=device, device_id_type=MESH
        )

    def wait_bytes(kib, sem):
        lines = pv.at[0, pl.ds(0, kib * 4)]
        pltpu.make_async_copy(lines, lines, sem).wait()

    half = WIDTH // 2
    loads = [
        pltpu.make_async_copy(q_hbm.at[:, :half], q_x.at[gx], q_load),
        pltpu.make_async_copy(q_hbm.at[:, half:], q_y.at[gy], q_load),
        pltpu.make_async_copy(ck_hbm, ck, k_load),
        pltpu.make_async_copy(cv_hbm, cv, v_load),
        pltpu.make_async_copy(pk_hbm, pk, pool_load),
        pltpu.make_async_copy(pv_hbm, pv, pool_load),
    ]
    smalls = [
        pltpu.make_async_copy(src, dst, small_load.at[i])
        for i, (src, dst) in enumerate(
            ((own_hbm, owns), (len_hbm, lens), (fill_hbm, fills), (free_hbm, frees))
        )
    ]

    def own_of(k):
        return core * (k // 4) + (1 - core) * (k % 2)

    def there_of(k):
        i = core * (k % 4) + (1 - core) * (k // 2)
        return (z + jnp.where(i == 0, 2, jnp.where(i == 1, 1, jnp.where(i == 2, 3, 0)))) % 4

    def block_of(k):
        own = own_of(k)
        return 2 * there_of(k) + own * core + (1 - own) * (1 - core)

    def w_copy(block):
        columns = pl.ds(pl.multiple_of(block * COLUMNS, COLUMNS), COLUMNS)
        return pltpu.make_async_copy(w_hbm.at[:, columns], w.at[block], w_load)

    loads[0].start()
    loads[1].start()
    smalls[0].start()
    barrier = pltpu.get_barrier_semaphore()
    for d in steps:
        pl.semaphore_signal(
            barrier, inc=1, device_id={"group": gy * 4 + (gx + d) % 4}, device_id_type=MESH
        )
        pl.semaphore_signal(
            barrier, inc=1, device_id={"group": (gy + d) % 4 * 4 + gx}, device_id_type=MESH
        )
        pl.semaphore_signal(
            barrier, inc=1, device_id={"tp": (z + d) % 4 * 2 + core}, device_id_type=MESH
        )
    pl.semaphore_signal(barrier, inc=1, device_id={"tp": 2 * z + 1 - core}, device_id_type=MESH)
    for copy in loads[2:] + smalls[1:]:
        copy.start()

    smalls[0].wait()
    asked = jnp.where(iota((8, 128), 0) < HALF_HEADS, owns[0], owns[1])
    asked = asked.astype(jnp.float32).astype(jnp.bfloat16)
    ask_x[gx] = asked
    ask_y[gy] = asked
    pltpu.make_async_copy(q_x.at[0:2], q_x.at[0:2], q_load).wait()
    pl.semaphore_wait(barrier, 3 * len(steps) + 1)
    started = []
    for d in steps:
        along_x, along_y = gy * 4 + (gx + d) % 4, (gy + d) % 4 * 4 + gx
        started += [
            remote(ask_x.at[gx], ask_x.at[gx], query_sem, group=along_x),
            remote(ask_y.at[gy], ask_y.at[gy], query_sem, group=along_y),
            remote(q_x.at[gx], q_x.at[gx], query_sem, group=along_x),
            remote(q_y.at[gy], q_y.at[gy], query_sem, group=along_y),
        ]
    for copy in started:
        copy.start()
    for block in range(TP):
        w_copy(block).start()

    for h in range(HALF_HEADS):
        lanes = slice(h * HEAD_DIM, (h + 1) * HEAD_DIM)
        qf[h * ROWS : (h + 1) * ROWS, :] = q_x[gx, :, lanes].astype(jnp.float32)
        other = h + HALF_HEADS
        qf[other * ROWS : (other + 1) * ROWS, :] = q_y[gy, :, lanes].astype(jnp.float32)
    loads[2].wait()
    for r in range(ROWS):
        query = qf[pl.ds(r, HEADS, stride=ROWS), :].astype(jnp.bfloat16)
        scores_all[r] = dot_nt(query, ck[r])

    wait_bytes(2 * 3 * (16 + 2), query_sem)

    rows_here = 4 * ROWS
    shape = (4 * 8, rows_here)
    head_of = iota(shape, 0) % HALF_HEADS
    lane = iota(shape, 1)

    def picked(asks, queries, row_of_lane):
        wanted = asks[...].reshape(4 * 8, 128)[:, :rows_here].astype(jnp.float32)
        match = wanted == row_of_lane.astype(jnp.float32)
        found = jnp.zeros((4 * 8, HEAD_DIM), jnp.float32)
        for h in range(HALF_HEADS):
            chosen = jnp.where(match & (head_of == h), 1.0, 0.0).astype(jnp.bfloat16)
            rows = queries[:, :, h * HEAD_DIM : (h + 1) * HEAD_DIM].reshape(rows_here, HEAD_DIM)
            found += dot(chosen, rows)
        return found.astype(jnp.bfloat16).reshape(4, 8, HEAD_DIM)

    pick_x[...] = picked(ask_y, q_x, lane + gy * rows_here)
    pick_y[...] = picked(ask_x, q_y, lane // ROWS * rows_here + lane % ROWS + gx * ROWS)
    for d in steps:
        other_x, other_y = (gx + d) % 4, (gy + d) % 4
        remote(pick_x.at[other_y], got_x.at[gy], pick_sem, group=other_y * 4 + gx).start()
        remote(pick_y.at[other_x], got_y.at[gx], pick_sem, group=gy * 4 + other_x).start()
    got_x[gy] = pick_x[gy]
    got_y[gx] = pick_y[gx]


    for copy in smalls[1:]:
        copy.wait()
    line = iota((2, 128), 0)
    lane = iota((2, 128), 1)
    base = (group % 8) * SLOT_PAIRS
    known = jnp.where((line == 1) & (lane == base), frees[0].astype(jnp.float32), 0.0)
    for u in range(SLOTS):
        in_slot = (lane >= base + u * HEADS) & (lane < base + (u + 1) * HEADS)
        known += jnp.where((line == 0) & in_slot, owns[u].astype(jnp.float32), 0.0)
    known_all[group] = known
    for peer in peers:
        remote(known_all.at[group], known_all.at[group], part_sem, group=peer).start()

    position = iota((HEADS, CAP), 1)
    for r in range(ROWS):
        pairs = slice(r * HEADS, (r + 1) * HEADS)
        scores = jnp.where(position < lens[r], scores_all[r] * SCALE, FAR_BELOW)
        high = jnp.max(scores, axis=1, keepdims=True)
        weights = jnp.exp2(scores - high)
        total = jnp.sum(weights, axis=1, keepdims=True)
        near_high[pairs, :] = jnp.broadcast_to(high, (HEADS, HEAD_DIM))
        near_total[pairs, :] = jnp.broadcast_to(total, (HEADS, HEAD_DIM))
        weights_all[r] = weights.astype(jnp.bfloat16)
    loads[3].wait()
    for r in range(ROWS):
        near_mixed[r * HEADS : (r + 1) * HEADS, :] = dot(weights_all[r], cv[r])
    pltpu.make_async_copy(w.at[0:2], w.at[0:2], pool_load).wait()

    wait_bytes(2 * 3 * 2, pick_sem)

    first = jnp.sum(got_x[...].astype(jnp.float32), axis=0)
    last = jnp.sum(got_y[...].astype(jnp.float32), axis=0)
    lane = iota((8, 128), 1)
    line = iota((8, 128), 0)
    place = iota((HEADS, BLOCK), 1)
    highs, totals = jnp.zeros((1, 128), jnp.float32), jnp.zeros((1, 128), jnp.float32)
    slot_scores, slot_weights = [], []
    for u in range(SLOTS):
        heads = slice(u * HALF_HEADS, (u + 1) * HALF_HEADS)
        query = jnp.concatenate([first[heads], last[heads]], axis=0).astype(jnp.bfloat16)
        slot_scores.append(dot_nt(query, pk[u]) * SCALE)
    for u in range(SLOTS):
        visible = place < fills[u]
        scores = jnp.where(visible, slot_scores[u], FAR_BELOW)
        high = jnp.max(scores, axis=1, keepdims=True)
        weights = jnp.where(visible, jnp.exp2(scores - high), 0.0)
        total = jnp.sum(weights, axis=1, keepdims=True)
        slot_weights.append(weights.astype(jnp.bfloat16))
        own_lane = lane == base + u * HEADS + line
        highs += jnp.sum(jnp.where(own_lane, high, 0.0), axis=0, keepdims=True)
        totals += jnp.sum(jnp.where(own_lane, total, 0.0), axis=0, keepdims=True)
    slot_mixed = [dot(slot_weights[u], pv[u]) for u in range(SLOTS)]
    table_all[group] = jnp.concatenate([highs, totals], axis=0)
    mixed_all[group] = jnp.concatenate(slot_mixed, axis=0).astype(jnp.bfloat16)

    for peer in peers:
        remote(mixed_all.at[group], mixed_all.at[group], part_sem, group=peer).start()
        remote(table_all.at[group], table_all.at[group], part_sem, group=peer).start()
    wait_bytes(len(peers) * (4 + 1 + 1), part_sem)

    middle = GROUPS // 2

    def joint(tables):
        low = sum((tables[g] for g in range(1, middle)), tables[0])
        top = sum((tables[g] for g in range(middle + 1, GROUPS)), tables[middle])
        return jnp.concatenate([low, top], axis=1)

    table, known = joint(table_all), joint(known_all)
    free_total = jnp.sum(known[1:2, :], axis=1, keepdims=True).astype(jnp.int32)
    free_ref[...] = jnp.broadcast_to(free_total, (8, 128))
    span = (PAIRS, GROUPS * SLOT_PAIRS)
    own_pair = iota(span, 0)
    slot_pair = iota(span, 1)
    own_row = (own_pair // HEADS + group * ROWS).astype(jnp.float32)
    matched = (own_pair % HEADS == slot_pair % HEADS) & (known[0:1, :] == own_row)
    highs = jnp.where(matched, table[0:1, :], FAR_BELOW)
    far_high = jnp.max(highs, axis=1, keepdims=True)
    factor = jnp.where(matched, jnp.exp2(highs - far_high), 0.0)
    far_total = jnp.sum(factor * table[1:2, :], axis=1, keepdims=True)
    coarse = factor.astype(jnp.bfloat16)
    fine = (factor - coarse.astype(jnp.float32)).astype(jnp.bfloat16)
    parts = mixed_all[...].reshape(GROUPS * SLOT_PAIRS, HEAD_DIM)
    far_mixed = dot(coarse, parts) + dot(fine, parts)
    near = near_high[...]
    peak = jnp.maximum(near, far_high)
    near_scale = jnp.exp2(near - peak)
    far_scale = jnp.exp2(far_high - peak)
    joined[...] = (near_scale * near_mixed[...] + far_scale * far_mixed) / (
        near_scale * near_total[...] + far_scale * far_total
    )
    attended_all[...] = jnp.concatenate(
        [joined[pl.ds(h, ROWS, stride=HEADS), :].astype(jnp.bfloat16) for h in range(HEADS)], axis=1
    )

    pltpu.make_async_copy(w, w, w_load).wait()
    got[UNUSED] = jnp.zeros((ROWS, COLUMNS), jnp.bfloat16)

    def turn(k, held):
        before = jnp.maximum(k - 1, 0)
        nothing = jnp.where(k == 0, 1, 0)
        own, there = (1 - nothing) * own_of(before), there_of(before)

        @pl.when(own == 1)
        def _():
            pltpu.make_async_copy(got.at[there], got.at[there], got_sem.at[there]).wait()

        product = dot(attended_all[...], w[block_of(k)])
        held += got[own * there + (1 - own) * UNUSED].astype(jnp.float32)
        sent[k] = held.astype(jnp.bfloat16)
        slot = own * (4 + z) + (1 - own) * there
        slot = nothing * LANDED + (1 - nothing) * slot
        pltpu.make_async_remote_copy(
            sent.at[k], got.at[slot], send_sem, got_sem.at[slot],
            device_id={"tp": own * (2 * there + core) + (1 - own) * (2 * z + 1 - core)},
            device_id_type=MESH,
        ).start()
        return product

    total = lax.fori_loop(0, TP, turn, jnp.zeros((ROWS, COLUMNS), jnp.float32))
    for slot in [z, LANDED] + [4 + (z + d) % 4 for d in (1, 3, 2)]:
        pltpu.make_async_copy(got.at[slot], got.at[slot], got_sem.at[slot]).wait()
    for slot in [z] + [4 + (z + d) % 4 for d in (1, 3, 2)]:
        total += got[slot].astype(jnp.float32)
    out_ref[...] = total

    wait_bytes(96 + 12 + 12 + 90 + 256, send_sem)


def finish(summed, free, out_ref, free_ref):
    out_ref[...] = summed[...].astype(jnp.bfloat16)
    free_ref[0] = free[0, 0]


def per_device(*args):
    bf16, f32 = jnp.bfloat16, jnp.float32
    dma = pltpu.SemaphoreType.DMA
    summed, free = pl.pallas_call(
        kernel,
        out_shape=(
            pltpu.VMEM((ROWS, COLUMNS), f32),
            pltpu.VMEM((8, 128), jnp.int32),
        ),
        in_specs=[pl.BlockSpec(memory_space=pltpu.HBM)] * 10,
        out_specs=(
            pl.BlockSpec(memory_space=pltpu.VMEM),
            pl.BlockSpec(memory_space=pltpu.VMEM),
        ),
        scratch_shapes=[
            pltpu.VMEM((4, ROWS, WIDTH // 2), bf16),
            pltpu.VMEM((4, ROWS, WIDTH // 2), bf16),
            pltpu.VMEM((4, 8, 128), bf16),
            pltpu.VMEM((4, 8, 128), bf16),
            pltpu.VMEM((4, 8, HEAD_DIM), bf16),
            pltpu.VMEM((4, 8, HEAD_DIM), bf16),
            pltpu.VMEM((4, 8, HEAD_DIM), bf16),
            pltpu.VMEM((4, 8, HEAD_DIM), bf16),
            pltpu.VMEM((ROWS, CAP, HEAD_DIM), bf16),
            pltpu.VMEM((ROWS, CAP, HEAD_DIM), bf16),
            pltpu.VMEM((SLOTS, BLOCK, HEAD_DIM), bf16),
            pltpu.VMEM((SLOTS, BLOCK, HEAD_DIM), bf16),
            pltpu.VMEM((TP, WIDTH, COLUMNS), bf16),
            pltpu.VMEM((PAIRS, HEAD_DIM), f32),
            pltpu.VMEM((ROWS, HEADS, CAP), f32),
            pltpu.VMEM((ROWS, HEADS, CAP), bf16),
            pltpu.VMEM((PAIRS, HEAD_DIM), f32),
            pltpu.VMEM((PAIRS, HEAD_DIM), f32),
            pltpu.VMEM((PAIRS, HEAD_DIM), f32),
            pltpu.VMEM((PAIRS, HEAD_DIM), f32),
            pltpu.VMEM((ROWS, WIDTH), bf16),
            pltpu.VMEM((GROUPS, SLOT_PAIRS, HEAD_DIM), bf16),
            pltpu.VMEM((GROUPS, 2, 128), f32),
            pltpu.VMEM((GROUPS, 2, 128), f32),
            pltpu.VMEM((TP, ROWS, COLUMNS), bf16),
            pltpu.VMEM((10, ROWS, COLUMNS), bf16),
            pltpu.SMEM((ROWS,), jnp.int32),
            pltpu.SMEM((SLOTS,), jnp.int32),
            pltpu.SMEM((SLOTS,), jnp.int32),
            pltpu.SMEM((1,), jnp.int32),
            dma,
            dma,
            dma,
            dma,
            dma((4,)),
            dma,
            dma,
            dma,
            dma,
            dma,
            dma((10,)),
        ],
        compiler_params=pltpu.CompilerParams(
            collective_id=0, has_side_effects=True, vmem_limit_bytes=60 * 1024 * 1024
        ),
    )(*args)
    return pl.pallas_call(
        finish,
        out_shape=(
            jax.ShapeDtypeStruct((ROWS, COLUMNS), bf16),
            jax.ShapeDtypeStruct((1,), jnp.int32),
        ),
        in_specs=[pl.BlockSpec(memory_space=pltpu.VMEM)] * 2,
        out_specs=(
            pl.BlockSpec(memory_space=pltpu.VMEM),
            pl.BlockSpec(memory_space=pltpu.SMEM),
        ),
        compiler_params=pltpu.CompilerParams(vmem_limit_bytes=1024 * 1024),
    )(
        pltpu.with_memory_space_constraint(summed, pltpu.VMEM),
        pltpu.with_memory_space_constraint(free, pltpu.VMEM),
    )


def solution(mesh):
    in_specs = (
        P("group", "tp"),
        P("group", None, "tp"),
        P("group", None, "tp"),
        P("group", None, "tp"),
        P("group", None, "tp"),
        P("group"),
        P("group"),
        P("group"),
        P("group"),
        P("tp", None),
    )
    out_specs = (P("group", "tp"), P())
    return jax.shard_map(
        per_device, mesh=mesh, in_specs=in_specs, out_specs=out_specs, check_vma=False
    )
```
